32 devices in a mesh: expert: 4 (over x, core), tensor: 8 (over z, y).
Axes of the slice: x: 2, y: 2, z: 4, core: 2. Of those that a mesh axis runs over, the one named last changes fastest.
Arguments:
- tokens: bfloat16 [128, 7168], P('expert', 'tensor'), may hold values from -6 to 6
- routes: int32 [128, 8], P('expert'), may hold values from 0 to 15, all different within a row; in each aligned block of 128 rows (0 to 127, 128 to 255, ...) at most 128 rows name the same one
- gates: bfloat16 [128, 8], P('expert'), may hold values from 0.099609375 to 0.59765625
- w_gate: bfloat16 [16, 2048, 7168], P('expert', 'tensor'), may hold values from -0.0625 to 0.0625
- w_up: bfloat16 [16, 2048, 7168], P('expert', 'tensor'), may hold values from -0.0625 to 0.0625
- w_down: bfloat16 [16, 2048, 7168], P('expert', None, 'tensor'), may hold values from -0.125 to 0.125
Outputs:
- moe_out: bfloat16 [128, 7168], P('expert', 'tensor')
The draws below stay inside these ranges and needn't reach their ends.
Inputs may be any that keep to these rules, and one draw needn't show every extreme that they name: `routes`: each row names 8 different experts. No expert is named by more than 128 of the 128 rows, and one expert is named by exactly 128 rows.
All inputs are finite; a program needn't handle non-finite values.
Results may differ from the reference program's by a relative error of at most 0.0049.
Values may be sent and summed in bfloat16 or wider, within the bound.
A program may use at most 128 MiB of HBM per device.

```python
import math
import jax
import jax.numpy as jnp
import numpy as np
from jax import lax

D = 7168
FF = 2048
TOPK = 8
EXPERTS = 16
TOKENS = 128
CAP = 128


def steps_of(own_key, extent, split, smallest, largest):
    def one(dim, blocks):
        steps = jax.random.uniform(jax.random.fold_in(jax.random.fold_in(own_key, 6), dim), (blocks,), jnp.float32, smallest / len(split), largest / len(split))
        return jnp.repeat(jnp.exp(steps), extent[dim] // blocks).reshape((-1,) + (1,) * (len(extent) - dim - 1))

    factor_of = one(*split[0])
    for cut in split[1:]:
        factor_of = factor_of * one(*cut)
    return factor_of


def shared_out(key, own, number, rows, count, top, limit, lean):
    ranking = jax.random.permutation(key, count)
    crowded, ordinary = load_shares(count, rows * top, limit, lean, True), load_shares(count, rows * top, limit, lean, False)
    places = jnp.arange(count)

    def named(sizes, offset_by):
        used = int((sizes > 0).sum())
        fixed = max(1, used // 4)
        passed = fixed + (places - fixed + offset_by * (used - fixed)) % max(1, count - fixed)
        return jnp.zeros((count,), jnp.int32).at[ranking[jnp.where(places < fixed, places, passed)]].set(jnp.asarray(sizes, jnp.int32))

    sizes = jnp.where(number % 4 == 0, named(crowded, number // 4), named(ordinary, number - number // 4 - 1))
    mixed = jax.random.permutation(jax.random.fold_in(own, 3), count)
    source_of, receiver = mixed[0:count // 2 * 2:2], mixed[1:count // 2 * 2:2]
    room = jnp.minimum(sizes[source_of] - 1, limit - sizes[receiver]) // 2
    room = jnp.where((source_of == ranking[0]) | (receiver == ranking[0]) | (sizes[receiver] == 0), 0, jnp.maximum(room, 0))
    passed = jax.random.randint(jax.random.fold_in(own, 4), (count // 2,), 0, 1 << 20) % (room + 1)
    sizes = sizes.at[source_of].add(-passed).at[receiver].add(passed)
    labels = jnp.searchsorted(jnp.cumsum(sizes), jnp.arange(rows * top), side="right").astype(jnp.int32)
    table = labels.reshape(top, rows).T
    table = table[jax.random.permutation(jax.random.fold_in(own, 1), rows)]
    offset_by = jax.random.randint(jax.random.fold_in(own, 2), (rows, 1), 0, top)
    return jnp.take_along_axis(table, (jnp.arange(top)[None, :] + offset_by) % top, axis=1)


def load_shares(count, total, limit, lean, full):
    weights = [(1 << 20) // math.isqrt(standing ** lean) + 1 for standing in range(1, count + 1)]
    largest = limit if full else min(limit, max(-(-total // count), total * weights[0] // sum(weights)))
    least = 1 if total - largest >= count - 1 else 0
    given, surplus = [largest] + [least] * (count - 1), total - largest - least * (count - 1)
    while surplus > 0:
        movable = [i for i in range(1, count) if given[i] < largest] or [i for i in range(1, count) if given[i] < limit]
        whole, remaining = sum([weights[i] for i in movable]), surplus
        for i in movable:
            more = min(limit - given[i], max(1, remaining * weights[i] // whole), surplus)
            given[i] = given[i] + more
            surplus = surplus - more
    return np.array(given)


def scatter_about(key, shape, width, bound, split=(), kind=jnp.bfloat16):
    values = width * jax.random.normal(key, shape, jnp.float32)
    if split:
        values = values * steps_of(key, shape, split, -0.22, 0.18)
    return jnp.clip(values, -bound, bound).astype(kind)


def setup_inputs(seed: int = 0) -> dict:
    arg_keys = jax.random.split(jax.random.key(seed), 7)
    tokens = scatter_about(arg_keys[0], (TOKENS, D), 1.0, 6.0, ((0, 4), (1, 8)))
    routes_keys = jax.random.split(jax.random.fold_in(arg_keys[1], 1), TOKENS // TOKENS)
    routes_turns = jax.random.permutation(jax.random.fold_in(arg_keys[1], 3), TOKENS // TOKENS)
    routes = jax.vmap(lambda own, number: shared_out(jax.random.fold_in(arg_keys[1], 2), own, number, TOKENS, EXPERTS, TOPK, CAP, 2))(routes_keys, routes_turns).reshape((TOKENS, TOPK))
    gates = jnp.clip(0.099609375 + 0.49804688 * jax.random.uniform(arg_keys[2], (TOKENS, TOPK), jnp.float32) ** steps_of(arg_keys[2], (TOKENS, TOPK), ((0, 4),), -0.2, 0.2), 0.099609375, 0.59765625).astype(jnp.bfloat16)
    w_gate = scatter_about(arg_keys[3], (EXPERTS, FF, D), D ** -0.5, 0.0625, ((0, 4), (1, 8)))
    w_up = scatter_about(arg_keys[4], (EXPERTS, FF, D), D ** -0.5, 0.0625, ((0, 4), (1, 8)))
    w_down = scatter_about(arg_keys[5], (EXPERTS, FF, D), FF ** -0.5, 0.125, ((0, 4), (2, 8)))
    return {"tokens": tokens, "routes": routes, "gates": gates, "w_gate": w_gate, "w_up": w_up, "w_down": w_down}


def reference(tokens, routes, gates, w_gate, w_up, w_down):
    expert_ids = jnp.arange(EXPERTS, dtype=jnp.int32)
    route_hits = routes[:, :, None] == expert_ids[None, None, :]
    member = jnp.sum(route_hits.astype(jnp.int32), axis=1)
    position = jnp.cumsum(member, axis=0) - member
    weights = jnp.sum(gates.astype(jnp.float32)[:, :, None] * route_hits.astype(jnp.float32), axis=1)
    slot_ids = jnp.arange(CAP, dtype=jnp.int32)

    def one_expert(running, packed):
        member_col, place_col, weight_col, gate_w, up_w, down_w = packed
        picked = (place_col[None, :] == slot_ids[:, None]) & (member_col[None, :] > 0)
        slot_rows = jnp.dot(picked.astype(jnp.bfloat16), tokens, preferred_element_type=jnp.float32).astype(jnp.bfloat16)
        gate_proj = lax.dot_general(slot_rows, gate_w, (((1,), (1,)), ((), ())), preferred_element_type=jnp.float32)
        up_proj = lax.dot_general(slot_rows, up_w, (((1,), (1,)), ((), ())), preferred_element_type=jnp.float32)
        hidden = (jax.nn.silu(gate_proj) * up_proj).astype(jnp.bfloat16)
        expert_out = jnp.dot(hidden, down_w, preferred_element_type=jnp.float32)
        mixing = picked.astype(jnp.float32).T * weight_col[:, None]
        return running + jnp.dot(mixing, expert_out, precision=lax.Precision.HIGHEST), None

    start = jnp.zeros((tokens.shape[0], tokens.shape[1]), jnp.float32)
    running, _ = lax.scan(one_expert, start, (member.T, position.T, weights.T, w_gate, w_up, w_down))
    return running.astype(jnp.bfloat16)
```

```python
import functools

import jax
import jax.numpy as jnp
from jax import lax
from jax.experimental import pallas as pl
from jax.experimental.pallas import tpu as pltpu
from jax.sharding import PartitionSpec as P

MESH = pl.DeviceIdType.MESH
LANES = 128
TRANSPOSED = (((1,), (1,)), ((), ()))


def token_weights(routes, gates, width):
    ids = lax.broadcasted_iota(jnp.int32, (routes.shape[0], width), 1)
    total = jnp.zeros((routes.shape[0], width), jnp.float32)
    for k in range(routes.shape[1]):
        total += jnp.where(routes[:, k : k + 1] == ids, gates[:, k : k + 1].astype(jnp.float32), 0.0)
    return total


def kernel(
    groups, parts, tokens, routes, gates, w_gate, w_up, w_down, out,
    x_all, wts, wg, wu, wd, hid, g_acc, u_acc, acc, outgoing, incoming,
    own_sem, wg_sem, wu_sem, wd_sem,
    x_send, x_recv, w_send, w_recv, h_send, h_recv, r_send, r_recv,
):
    exp_dev, ff_blk, width = w_gate.shape
    rows, d_blk = tokens.shape
    n_x, n_z = groups // 2, parts // 2
    me_e, me_t = lax.axis_index("expert"), lax.axis_index("tensor")
    xi, ci, zi, yi = me_e // 2, me_e % 2, me_t // 2, me_t % 2

    def group_at(m, o):
        return lax.rem(xi + m, n_x) * 2 + (ci if o == 0 else 1 - ci)

    def part_at(k, o):
        return lax.rem(zi + k, n_z) * 2 + (yi if o == 0 else 1 - yi)

    def row_slice(g):
        return pl.ds(pl.multiple_of(g * rows, rows), rows)

    own = x_all.at[row_slice(me_e), pl.ds(pl.multiple_of(me_t * d_blk, LANES), d_blk)]
    own_copy = pltpu.make_async_copy(tokens, own, own_sem)
    own_copy.start()
    loads_g, loads_u, loads_d = [], [], []
    for e in range(exp_dev):
        loads_g.append(pltpu.make_async_copy(w_gate.at[e], wg.at[e], wg_sem.at[e]))
        loads_u.append(pltpu.make_async_copy(w_up.at[e], wu.at[e], wu_sem.at[e]))
        loads_d.append(pltpu.make_async_copy(w_down.at[e], wd.at[e], wd_sem.at[e]))
    for e in range(exp_dev):
        loads_g[e].start()
        loads_u[e].start()

    z_peers = [(me_e, part_at(k, 0)) for k in range(1, n_z)]
    y_peer = (me_e, part_at(0, 1))
    others = [(m, o) for m in range(n_x) for o in range(2) if (m, o) != (0, 0)]
    e_peers = [(group_at(m, o), me_t) for m, o in others]
    barrier = pltpu.get_barrier_semaphore()
    for peer in z_peers + [y_peer] + e_peers:
        pl.semaphore_signal(barrier, inc=1, device_id=peer, device_id_type=MESH)
    wts[row_slice(me_e), :] = token_weights(routes[...], gates[...], wts.shape[1])
    pl.semaphore_wait(barrier, len(z_peers) + 1 + len(e_peers))

    started = []

    def send(src, dst, send_sem, recv_sem, peer):
        copy = pltpu.make_async_remote_copy(
            src_ref=src, dst_ref=dst, send_sem=send_sem, recv_sem=recv_sem,
            device_id=peer, device_id_type=MESH,
        )
        copy.start()
        started.append(copy)

    def arrived(dst, recv_sem):
        pltpu.make_async_remote_copy(
            src_ref=dst, dst_ref=dst, send_sem=own_sem, recv_sem=recv_sem,
            device_id=y_peer, device_id_type=MESH,
        ).wait_recv()

    def block(m, o, k, yo):
        g, t = group_at(m, o), part_at(k, yo)
        return x_all.at[row_slice(g), pl.ds(pl.multiple_of(t * d_blk, LANES), d_blk)]

    def sem_z(k):
        return k - 1

    def sem_y(k):
        return n_z - 1 + k

    def sem_x(m, k, yo):
        return 2 * n_z - 1 + (m - 1) * parts + k * 2 + yo

    def sem_c(m, k, yo):
        return 2 * n_z - 1 + (n_x - 1) * parts + m * parts + k * 2 + yo

    def to_x(k, yo):
        b = block(0, 0, k, yo)
        for m in range(1, n_x):
            send(b, b, x_send.at[sem_x(m, k, yo)], x_recv.at[sem_x(n_x - m, k, yo)], (group_at(m, 0), me_t))

    def to_core(m, k, yo):
        b = block(m, 0, k, yo)
        s = sem_c(m, k, yo)
        send(b, b, x_send.at[s], x_recv.at[s], (group_at(0, 1), me_t))

    def to_y(k):
        b = block(0, 0, k, 0)
        send(b, b, x_send.at[sem_y(k)], x_recv.at[sem_y(k)], y_peer)

    own_copy.wait()
    first = block(0, 0, 0, 0)
    for k in range(1, n_z):
        send(first, first, x_send.at[sem_z(k)], x_recv.at[sem_z(n_z - k)], z_peers[k - 1])
    to_y(0)
    to_x(0, 0)
    to_core(0, 0, 0)
    mine = wts.at[row_slice(me_e), :]
    for (m, o), peer in zip(others, e_peers):
        back = ((n_x - m) % n_x) * 2 + o
        send(mine, mine, w_send.at[m * 2 + o], w_recv.at[back], peer)
    for e in range(exp_dev):
        loads_d[e].start()
    for k in range(1, n_z):
        arrived(block(0, 0, k, 0), x_recv.at[sem_z(k)])
        to_y(k)
        to_x(k, 0)
        to_core(0, k, 0)
    for k in range(n_z):
        arrived(block(0, 0, k, 1), x_recv.at[sem_y(k)])
        to_x(k, 1)
        to_core(0, k, 1)
    for yo in range(2):
        for k in range(n_z):
            for m in range(1, n_x):
                arrived(block(m, 0, k, yo), x_recv.at[sem_x(m, k, yo)])
                to_core(m, k, yo)
    for m, o in others:
        arrived(wts.at[row_slice(group_at(m, o)), :], w_recv.at[m * 2 + o])
    for m in range(n_x):
        for yo in range(2):
            for k in range(n_z):
                arrived(block(m, 1, k, yo), x_recv.at[sem_c(m, k, yo)])

    steps = 4 if width % (4 * 2 * LANES) == 0 else 1
    k_blk = width // steps

    def compute(e):
        loads_g[e].wait()
        loads_u[e].wait()
        g_acc[...] = jnp.zeros_like(g_acc)
        u_acc[...] = jnp.zeros_like(u_acc)

        def step(i, carry):
            cols = pl.ds(pl.multiple_of(i * k_blk, LANES), k_blk)
            x = x_all[:, cols]
            g_acc[...] += lax.dot_general(x, wg[e, :, cols], TRANSPOSED, preferred_element_type=jnp.float32)
            u_acc[...] += lax.dot_general(x, wu[e, :, cols], TRANSPOSED, preferred_element_type=jnp.float32)
            return carry

        lax.fori_loop(0, steps, step, 0)
        ids = lax.broadcasted_iota(jnp.int32, wts.shape, 1)
        weight = jnp.sum(jnp.where(ids == me_e * exp_dev + e, wts[...], 0.0), axis=1, keepdims=True)
        g = g_acc[...]
        hid[me_t, e] = (g / (1.0 + jnp.exp(-g)) * u_acc[...] * weight).astype(hid.dtype)

    def h_sem_z(k, e):
        return (k - 1) * exp_dev + e

    def h_sem_y(k, e):
        return (n_z - 1 + k) * exp_dev + e

    def h_to_y(k, e):
        b = hid.at[part_at(k, 0), e]
        send(b, b, h_send.at[h_sem_y(k, e)], h_recv.at[h_sem_y(k, e)], y_peer)

    def h_own(e):
        b = hid.at[me_t, e]
        h_to_y(0, e)
        for k in range(1, n_z):
            send(b, b, h_send.at[h_sem_z(k, e)], h_recv.at[h_sem_z(n_z - k, e)], z_peers[k - 1])

    def h_forward(e):
        for k in range(1, n_z):
            arrived(hid.at[part_at(k, 0), e], h_recv.at[h_sem_z(k, e)])
            h_to_y(k, e)

    def down(e, yo):
        def step(k, carry):
            t = lax.rem(zi + k, n_z) * 2 + (yi if yo == 0 else 1 - yi)
            w = wd[e, pl.ds(pl.multiple_of(t * ff_blk, ff_blk), ff_blk), :]
            acc[...] += jnp.dot(hid[t, e], w, preferred_element_type=jnp.float32)
            return carry

        lax.fori_loop(0, n_z, step, 0)

    def down_z(e):
        loads_d[e].wait()
        down(e, 0)

    def down_y(e):
        for k in range(n_z):
            arrived(hid.at[part_at(k, 1), e], h_recv.at[h_sem_y(k, e)])
        down(e, 1)

    acc[...] = jnp.zeros_like(acc)
    for e in range(exp_dev):
        compute(e)
        h_own(e)
        if e >= 2:
            h_forward(e - 2)
    late = range(max(exp_dev - 2, 0), exp_dev)
    for e in late:
        if e >= 2:
            down_z(e - 2)
        h_forward(e)
    for e in range(exp_dev):
        if e + 2 not in late:
            down_z(e)
    for e in range(exp_dev):
        down_y(e)

    for (m, o), peer in zip(others, e_peers):
        i = m * 2 + o
        outgoing[i] = acc[row_slice(group_at(m, o)), :].astype(outgoing.dtype)
        back = ((n_x - m) % n_x) * 2 + o
        send(outgoing.at[i], incoming.at[back], r_send.at[i], r_recv.at[back], peer)
    total = acc[row_slice(me_e), :]
    for m, o in others:
        arrived(incoming.at[m * 2 + o], r_recv.at[m * 2 + o])
    for m, o in others:
        total += incoming[m * 2 + o].astype(jnp.float32)
    out[...] = total.astype(out.dtype)
    for copy in started:
        copy.wait_send()


def fused(groups, parts, tokens, routes, gates, w_gate, w_up, w_down):
    exp_dev, ff_blk, width = w_gate.shape
    rows, d_blk = tokens.shape
    all_rows, experts = rows * groups, exp_dev * groups
    n_x, n_z = groups // 2, parts // 2
    x_copies = 2 * n_z - 1 + (n_x - 1) * parts + n_x * parts
    h_copies = (2 * n_z - 1) * exp_dev
    dma, kind = pltpu.SemaphoreType.DMA, tokens.dtype
    any_spec, vmem_spec = pl.BlockSpec(memory_space=pl.ANY), pl.BlockSpec(memory_space=pltpu.VMEM)
    return pl.pallas_call(
        functools.partial(kernel, groups, parts),
        out_shape=jax.ShapeDtypeStruct((rows, d_blk), kind),
        in_specs=[any_spec, vmem_spec, vmem_spec, any_spec, any_spec, any_spec],
        out_specs=vmem_spec,
        scratch_shapes=[
            pltpu.VMEM((all_rows, width), kind),
            pltpu.VMEM((all_rows, -(-experts // LANES) * LANES), jnp.float32),
            pltpu.VMEM(w_gate.shape, kind),
            pltpu.VMEM(w_up.shape, kind),
            pltpu.VMEM(w_down.shape, kind),
            pltpu.VMEM((parts, exp_dev, all_rows, ff_blk), kind),
            pltpu.VMEM((all_rows, ff_blk), jnp.float32),
            pltpu.VMEM((all_rows, ff_blk), jnp.float32),
            pltpu.VMEM((all_rows, d_blk), jnp.float32),
            pltpu.VMEM((groups, rows, d_blk), kind),
            pltpu.VMEM((groups, rows, d_blk), kind),
            dma, dma((exp_dev,)), dma((exp_dev,)), dma((exp_dev,)),
            dma((x_copies,)), dma((x_copies,)),
            dma((groups,)), dma((groups,)),
            dma((h_copies,)), dma((h_copies,)),
            dma((groups,)), dma((groups,)),
        ],
        compiler_params=pltpu.CompilerParams(
            collective_id=0, has_side_effects=True, vmem_limit_bytes=60 * 1024 * 1024
        ),
        name="moe_decode",
    )(tokens, routes, gates, w_gate, w_up, w_down)


def plain(groups, tokens, routes, gates, w_gate, w_up, w_down):
    exp_dev = w_gate.shape[0]
    weights = token_weights(routes, gates, exp_dev * groups)
    weights = lax.all_gather(weights, "expert", axis=0, tiled=True)
    own = lax.dynamic_slice_in_dim(weights, lax.axis_index("expert") * exp_dev, exp_dev, axis=1)
    row_block = lax.all_gather(tokens, "expert", axis=0, tiled=True)
    x = lax.all_gather(row_block, "tensor", axis=1, tiled=True)
    gate_proj = jnp.einsum("nd,efd->enf", x, w_gate, preferred_element_type=jnp.float32)
    up_proj = jnp.einsum("nd,efd->enf", x, w_up, preferred_element_type=jnp.float32)
    hidden = (jax.nn.silu(gate_proj) * up_proj * own.T[:, :, None]).astype(jnp.bfloat16)
    hidden = lax.all_gather(hidden, "tensor", axis=2, tiled=True)
    partial = jnp.einsum("enf,efd->nd", hidden, w_down, preferred_element_type=jnp.float32)
    return lax.psum_scatter(partial, "expert", scatter_dimension=0, tiled=True).astype(tokens.dtype)


def solution(mesh):
    groups, parts = mesh.shape["expert"], mesh.shape["tensor"]

    def on_device(tokens, routes, gates, w_gate, w_up, w_down):
        tiles = tokens.shape[1] % LANES == 0 and w_gate.shape[1] % LANES == 0 and tokens.shape[0] % 16 == 0
        if tiles and groups % 2 == 0 and parts % 2 == 0:
            return fused(groups, parts, tokens, routes, gates, w_gate, w_up, w_down)
        return plain(groups, tokens, routes, gates, w_gate, w_up, w_down)

    placed = (
        P("expert", "tensor"),
        P("expert", None),
        P("expert", None),
        P("expert", "tensor", None),
        P("expert", "tensor", None),
        P("expert", None, "tensor"),
    )
    return jax.shard_map(
        on_device, mesh=mesh, in_specs=placed, out_specs=P("expert", "tensor"), check_vma=False
    )
```

```python
import functools

import jax
import jax.numpy as jnp
from jax import lax
from jax.experimental import pallas as pl
from jax.experimental.pallas import tpu as pltpu
from jax.sharding import PartitionSpec as P

MESH = pl.DeviceIdType.MESH
LANES = 128
TRANSPOSED = (((1,), (1,)), ((), ()))


def token_weights(routes, gates, width):
    ids = lax.broadcasted_iota(jnp.int32, (routes.shape[0], width), 1)
    total = jnp.zeros((routes.shape[0], width), jnp.float32)
    for k in range(routes.shape[1]):
        total += jnp.where(routes[:, k : k + 1] == ids, gates[:, k : k + 1].astype(jnp.float32), 0.0)
    return total


def kernel(
    groups, parts, tokens, routes, gates, w_gate, w_up, w_down, out,
    x_all, wts, wg, wu, wd, hid, g_acc, u_acc, acc, outgoing, incoming,
    own_sem, wg_sem, wu_sem, wd_sem,
    x_send, x_recv, w_send, w_recv, h_send, h_recv, r_send, r_recv,
):
    exp_dev, ff_blk, width = w_gate.shape
    rows, d_blk = tokens.shape
    n_x, n_z = groups // 2, parts // 2
    bits = [1 << i for i in range((n_z - 1).bit_length())]
    me_e, me_t = lax.axis_index("expert"), lax.axis_index("tensor")
    xi, ci, zi, yi = me_e // 2, me_e % 2, me_t // 2, me_t % 2

    def group_at(m, o):
        return lax.rem(xi + m, n_x) * 2 + (ci if o == 0 else 1 - ci)

    def part_at(k, o):
        z = zi
        for bit in bits:
            if k & bit:
                z = z + bit - 2 * bit * ((zi // bit) % 2)
        return z * 2 + (yi if o == 0 else 1 - yi)

    def row_slice(g):
        return pl.ds(pl.multiple_of(g * rows, rows), rows)

    own = x_all.at[row_slice(me_e), pl.ds(pl.multiple_of(me_t * d_blk, LANES), d_blk)]
    own_copy = pltpu.make_async_copy(tokens, own, own_sem)
    own_copy.start()
    loads_g, loads_u, loads_d = [], [], []
    for e in range(exp_dev):
        loads_g.append(pltpu.make_async_copy(w_gate.at[e], wg.at[e], wg_sem.at[e]))
        loads_u.append(pltpu.make_async_copy(w_up.at[e], wu.at[e], wu_sem.at[e]))
        loads_d.append(pltpu.make_async_copy(w_down.at[e], wd.at[e], wd_sem.at[e]))
    for e in range(exp_dev):
        loads_g[e].start()
        loads_u[e].start()

    z_peers = [(me_e, part_at(k, 0)) for k in range(1, n_z)]
    y_peer = (me_e, part_at(0, 1))
    others = [(m, o) for m in range(n_x) for o in range(2) if (m, o) != (0, 0)]
    e_peers = [(group_at(m, o), me_t) for m, o in others]
    barrier = pltpu.get_barrier_semaphore()
    for peer in z_peers + [y_peer] + e_peers:
        pl.semaphore_signal(barrier, inc=1, device_id=peer, device_id_type=MESH)
    wts[row_slice(me_e), :] = token_weights(routes[...], gates[...], wts.shape[1])
    pl.semaphore_wait(barrier, len(z_peers) + 1 + len(e_peers))

    started = []

    def send(src, dst, send_sem, recv_sem, peer):
        copy = pltpu.make_async_remote_copy(
            src_ref=src, dst_ref=dst, send_sem=send_sem, recv_sem=recv_sem,
            device_id=peer, device_id_type=MESH,
        )
        copy.start()
        started.append(copy)

    def arrived(dst, recv_sem):
        pltpu.make_async_remote_copy(
            src_ref=dst, dst_ref=dst, send_sem=own_sem, recv_sem=recv_sem,
            device_id=y_peer, device_id_type=MESH,
        ).wait_recv()

    def block(m, o, k, yo):
        g, t = group_at(m, o), part_at(k, yo)
        return x_all.at[row_slice(g), pl.ds(pl.multiple_of(t * d_blk, LANES), d_blk)]

    def sem_z(k):
        return k - 1

    def sem_y(k):
        return n_z - 1 + k

    def sem_x(m, k, yo):
        return 2 * n_z - 1 + (m - 1) * parts + k * 2 + yo

    def sem_c(m, k, yo):
        return 2 * n_z - 1 + (n_x - 1) * parts + m * parts + k * 2 + yo

    def to_x(k, yo):
        b = block(0, 0, k, yo)
        for m in range(1, n_x):
            send(b, b, x_send.at[sem_x(m, k, yo)], x_recv.at[sem_x(n_x - m, k, yo)], (group_at(m, 0), me_t))

    def to_core(m, k, yo):
        b = block(m, 0, k, yo)
        s = sem_c(m, k, yo)
        send(b, b, x_send.at[s], x_recv.at[s], (group_at(0, 1), me_t))

    def to_y(k):
        b = block(0, 0, k, 0)
        send(b, b, x_send.at[sem_y(k)], x_recv.at[sem_y(k)], y_peer)

    own_copy.wait()
    first = block(0, 0, 0, 0)
    for k in range(1, n_z):
        send(first, first, x_send.at[sem_z(k)], x_recv.at[sem_z(k)], z_peers[k - 1])
    to_y(0)
    to_x(0, 0)
    to_core(0, 0, 0)
    mine = wts.at[row_slice(me_e), :]
    for (m, o), peer in zip(others, e_peers):
        back = ((n_x - m) % n_x) * 2 + o
        send(mine, mine, w_send.at[m * 2 + o], w_recv.at[back], peer)
    for e in range(exp_dev):
        loads_d[e].start()
    for k in range(1, n_z):
        arrived(block(0, 0, k, 0), x_recv.at[sem_z(k)])
        to_y(k)
        to_x(k, 0)
        to_core(0, k, 0)
    for k in range(n_z):
        arrived(block(0, 0, k, 1), x_recv.at[sem_y(k)])
        to_x(k, 1)
        to_core(0, k, 1)
    for yo in range(2):
        for k in range(n_z):
            for m in range(1, n_x):
                arrived(block(m, 0, k, yo), x_recv.at[sem_x(m, k, yo)])
                to_core(m, k, yo)
    for m, o in others:
        arrived(wts.at[row_slice(group_at(m, o)), :], w_recv.at[m * 2 + o])
    for m in range(n_x):
        for yo in range(2):
            for k in range(n_z):
                arrived(block(m, 1, k, yo), x_recv.at[sem_c(m, k, yo)])

    steps = 4 if width % (4 * 2 * LANES) == 0 else 1
    k_blk = width // steps

    def compute(e):
        loads_g[e].wait()
        loads_u[e].wait()
        g_acc[...] = jnp.zeros_like(g_acc)
        u_acc[...] = jnp.zeros_like(u_acc)

        def step(i, carry):
            cols = pl.ds(pl.multiple_of(i * k_blk, LANES), k_blk)
            x = x_all[:, cols]
            g_acc[...] += lax.dot_general(x, wg[e, :, cols], TRANSPOSED, preferred_element_type=jnp.float32)
            u_acc[...] += lax.dot_general(x, wu[e, :, cols], TRANSPOSED, preferred_element_type=jnp.float32)
            return carry

        lax.fori_loop(0, steps, step, 0)
        ids = lax.broadcasted_iota(jnp.int32, wts.shape, 1)
        weight = jnp.sum(jnp.where(ids == me_e * exp_dev + e, wts[...], 0.0), axis=1, keepdims=True)
        g = g_acc[...]
        hid[me_t, e] = (g / (1.0 + jnp.exp(-g)) * u_acc[...] * weight).astype(hid.dtype)

    def h_sem_z(k, e):
        return (k - 1) * exp_dev + e

    def h_sem_y(k, e):
        return (n_z - 1 + k) * exp_dev + e

    def h_to_y(k, e):
        b = hid.at[part_at(k, 0), e]
        send(b, b, h_send.at[h_sem_y(k, e)], h_recv.at[h_sem_y(k, e)], y_peer)

    def h_own(e):
        b = hid.at[me_t, e]
        h_to_y(0, e)
        for k in reversed(bits):
            h_to_z(b, k, k, e)

    def h_to_z(b, step, role, e):
        s = h_sem_z(role, e)
        send(b, b, h_send.at[s], h_recv.at[s], z_peers[step - 1])

    def h_take(k, e):
        b = hid.at[part_at(k, 0), e]
        arrived(b, h_recv.at[h_sem_z(k, e)])
        for bit in reversed(bits):
            if bit < (k & -k):
                h_to_z(b, bit, k | bit, e)
        h_to_y(k, e)

    def h_relay(e):
        for k in reversed(bits):
            h_take(k, e)

    def h_forward(e):
        for k in sorted(range(1, n_z), key=lambda k: -(k & -k)):
            if k not in bits:
                h_take(k, e)

    def down(e, yo):
        def step(k, carry):
            t = k * 2 + (yi if yo == 0 else 1 - yi)
            w = wd[e, pl.ds(pl.multiple_of(t * ff_blk, ff_blk), ff_blk), :]
            acc[...] += jnp.dot(hid[t, e], w, preferred_element_type=jnp.float32)
            return carry

        lax.fori_loop(0, n_z, step, 0)

    def down_z(e):
        loads_d[e].wait()
        down(e, 0)

    def down_y(e):
        for k in range(n_z):
            arrived(hid.at[part_at(k, 1), e], h_recv.at[h_sem_y(k, e)])
        down(e, 1)

    acc[...] = jnp.zeros_like(acc)
    for e in range(exp_dev):
        compute(e)
        h_own(e)
        if e >= 1:
            h_relay(e - 1)
        if e >= 2:
            h_forward(e - 2)
    h_relay(exp_dev - 1)
    if exp_dev >= 2:
        h_forward(exp_dev - 2)
    for e in range(exp_dev - 1):
        down_z(e)
    h_forward(exp_dev - 1)
    down_z(exp_dev - 1)
    for e in range(exp_dev):
        down_y(e)

    for (m, o), peer in zip(others, e_peers):
        i = m * 2 + o
        outgoing[i] = acc[row_slice(group_at(m, o)), :].astype(outgoing.dtype)
        back = ((n_x - m) % n_x) * 2 + o
        send(outgoing.at[i], incoming.at[back], r_send.at[i], r_recv.at[back], peer)
    total = acc[row_slice(me_e), :]
    for m, o in others:
        arrived(incoming.at[m * 2 + o], r_recv.at[m * 2 + o])
    for m, o in others:
        total += incoming[m * 2 + o].astype(jnp.float32)
    out[...] = total.astype(out.dtype)
    for copy in started:
        copy.wait_send()


def fused(groups, parts, tokens, routes, gates, w_gate, w_up, w_down):
    exp_dev, ff_blk, width = w_gate.shape
    rows, d_blk = tokens.shape
    all_rows, experts = rows * groups, exp_dev * groups
    n_x, n_z = groups // 2, parts // 2
    x_copies = 2 * n_z - 1 + (n_x - 1) * parts + n_x * parts
    h_copies = (2 * n_z - 1) * exp_dev
    dma, kind = pltpu.SemaphoreType.DMA, tokens.dtype
    any_spec, vmem_spec = pl.BlockSpec(memory_space=pl.ANY), pl.BlockSpec(memory_space=pltpu.VMEM)
    return pl.pallas_call(
        functools.partial(kernel, groups, parts),
        out_shape=jax.ShapeDtypeStruct((rows, d_blk), kind),
        in_specs=[any_spec, vmem_spec, vmem_spec, any_spec, any_spec, any_spec],
        out_specs=vmem_spec,
        scratch_shapes=[
            pltpu.VMEM((all_rows, width), kind),
            pltpu.VMEM((all_rows, -(-experts // LANES) * LANES), jnp.float32),
            pltpu.VMEM(w_gate.shape, kind),
            pltpu.VMEM(w_up.shape, kind),
            pltpu.VMEM(w_down.shape, kind),
            pltpu.VMEM((parts, exp_dev, all_rows, ff_blk), kind),
            pltpu.VMEM((all_rows, ff_blk), jnp.float32),
            pltpu.VMEM((all_rows, ff_blk), jnp.float32),
            pltpu.VMEM((all_rows, d_blk), jnp.float32),
            pltpu.VMEM((groups, rows, d_blk), kind),
            pltpu.VMEM((groups, rows, d_blk), kind),
            dma, dma((exp_dev,)), dma((exp_dev,)), dma((exp_dev,)),
            dma((x_copies,)), dma((x_copies,)),
            dma((groups,)), dma((groups,)),
            dma((h_copies,)), dma((h_copies,)),
            dma((groups,)), dma((groups,)),
        ],
        compiler_params=pltpu.CompilerParams(
            collective_id=0, has_side_effects=True, vmem_limit_bytes=60 * 1024 * 1024
        ),
        name="moe_decode",
    )(tokens, routes, gates, w_gate, w_up, w_down)


def plain(groups, tokens, routes, gates, w_gate, w_up, w_down):
    exp_dev = w_gate.shape[0]
    weights = token_weights(routes, gates, exp_dev * groups)
    weights = lax.all_gather(weights, "expert", axis=0, tiled=True)
    own = lax.dynamic_slice_in_dim(weights, lax.axis_index("expert") * exp_dev, exp_dev, axis=1)
    row_block = lax.all_gather(tokens, "expert", axis=0, tiled=True)
    x = lax.all_gather(row_block, "tensor", axis=1, tiled=True)
    gate_proj = jnp.einsum("nd,efd->enf", x, w_gate, preferred_element_type=jnp.float32)
    up_proj = jnp.einsum("nd,efd->enf", x, w_up, preferred_element_type=jnp.float32)
    hidden = (jax.nn.silu(gate_proj) * up_proj * own.T[:, :, None]).astype(jnp.bfloat16)
    hidden = lax.all_gather(hidden, "tensor", axis=2, tiled=True)
    partial = jnp.einsum("enf,efd->nd", hidden, w_down, preferred_element_type=jnp.float32)
    return lax.psum_scatter(partial, "expert", scatter_dimension=0, tiled=True).astype(tokens.dtype)


def solution(mesh):
    groups, parts = mesh.shape["expert"], mesh.shape["tensor"]

    def on_device(tokens, routes, gates, w_gate, w_up, w_down):
        tiles = tokens.shape[1] % LANES == 0 and w_gate.shape[1] % LANES == 0 and tokens.shape[0] % 16 == 0
        if tiles and groups % 2 == 0 and parts > 1 and parts & (parts - 1) == 0:
            return fused(groups, parts, tokens, routes, gates, w_gate, w_up, w_down)
        return plain(groups, tokens, routes, gates, w_gate, w_up, w_down)

    placed = (
        P("expert", "tensor"),
        P("expert", None),
        P("expert", None),
        P("expert", "tensor", None),
        P("expert", "tensor", None),
        P("expert", None, "tensor"),
    )
    return jax.shard_map(
        on_device, mesh=mesh, in_specs=placed, out_specs=P("expert", "tensor"), check_vma=False
    )
```
